32 devices in a mesh: groups: 2 (over x), expert: 16 (over z, y, core).
Axes of the slice: x: 2, y: 2, z: 4, core: 2. Of those that a mesh axis runs over, the one named last changes fastest.
Arguments:
- tokens: bfloat16 [4096, 7168], P(('groups', 'expert')), parts along dimension 0, may hold values from -6 to 6
- route_ids: int32 [4096, 2], P(('groups', 'expert')), parts along dimension 0, may hold values from 0 to 3, all different within a row; in each aligned block of 128 rows (0 to 127, 128 to 255, ...) at most 80 rows name the same one
- levels: int32 [4096, 2], P(('groups', 'expert')), parts along dimension 0, may hold values from 1 to 64
- w_gate: bfloat16 [16, 7168, 512], P('expert'), may hold values from -0.0625 to 0.0625
- w_up: bfloat16 [16, 7168, 512], P('expert'), may hold values from -0.0625 to 0.0625
- w_down: bfloat16 [16, 512, 7168], P('expert'), may hold values from -0.125 to 0.125
Outputs:
- combined: bfloat16 [4096, 7168], P(('groups', 'expert')), parts along dimension 0
The draws below stay inside these ranges and needn't reach their ends.
There are 2 independent parts, one for each index of `groups`. The reference program is written for one: setup_inputs(seed, part) draws one part's arguments, and reference() takes and returns one part's arrays. A program takes and returns all parts, laid end to end along the dimension named above; an argument that names none is the same for every part. Nothing has to cross between parts.
Inputs may be any that keep to these rules, and one draw needn't show every extreme that they name: `route_ids`: each row names 2 different experts; among the rows of one device no expert is named more than 80 times, a bound that some block reaches.
All inputs are finite; a program needn't handle non-finite values.
Results may differ from the reference program's by a relative error of at most 0.013.
Values may be sent and summed in bfloat16 or wider, within the bound.
No kernel may reach another device: no remote copies, remote signals or barrier semaphores. Data moves between devices by JAX's collectives and lax.ppermute only.
A program may use at most 192 MiB of HBM per device.

```python
import math
import jax
import jax.numpy as jnp
import numpy as np
from jax import lax

D = 7168
FF_WIN = 2048
SHARDS = 4
FF_DEV = 512
TOK_DEV = 128
TOP = 2
EXPERTS = 4
CAP = 80
TOKENS = 2048
N_EXPERT = 16


def set_ends(values, rng, smallest, high):
    spot = [jax.random.randint(jax.random.fold_in(rng, axis), (), 0, length) for axis, length in enumerate(values.shape)]
    longest = values.shape.index(max(values.shape))
    neighbour = spot[:longest] + [(spot[longest] + 1) % values.shape[longest]] + spot[longest + 1:]
    return values.at[tuple(spot)].set(smallest).at[tuple(neighbour)].set(high)


def steps_of(own_key, extent, split, low, high):
    level, own = 1.0, jax.random.fold_in(own_key, 6)
    for position, shards_of in split:
        heights = jnp.exp(jax.random.uniform(jax.random.fold_in(own, position), (shards_of,), jnp.float32, low / len(split), high / len(split)))
        level = level * jnp.repeat(heights, extent[position] // shards_of).reshape([-1 if axis == position else 1 for axis in range(len(extent))])
    return level


def shared_out(key, own, number, rows, count, top, limit, slope):
    sequence = jax.random.permutation(key, count)
    packed, usual = portions_of(count, rows * top, limit, slope, True), portions_of(count, rows * top, limit, slope, False)
    places = jnp.arange(count)

    def named(tallies, offset_by):
        used = int((tallies > 0).sum())
        fixed = max(1, used // 4)
        shifted = fixed + (places - fixed + offset_by * (used - fixed)) % max(1, count - fixed)
        return jnp.zeros((count,), jnp.int32).at[sequence[jnp.where(places < fixed, places, shifted)]].set(jnp.asarray(tallies, jnp.int32))

    tallies = jnp.where(number % 4 == 0, named(packed, number // 4), named(usual, number - number // 4 - 1))
    mixed = jax.random.permutation(jax.random.fold_in(own, 3), count)
    donor, sink = mixed[0:count // 2 * 2:2], mixed[1:count // 2 * 2:2]
    margin = jnp.minimum(tallies[donor] - 1, limit - tallies[sink]) // 2
    margin = jnp.where((donor == sequence[0]) | (sink == sequence[0]) | (tallies[sink] == 0), 0, jnp.maximum(margin, 0))
    shifted = jax.random.randint(jax.random.fold_in(own, 4), (count // 2,), 0, 1 << 20) % (margin + 1)
    tallies = tallies.at[donor].add(-shifted).at[sink].add(shifted)
    members = jnp.searchsorted(jnp.cumsum(tallies), jnp.arange(rows * top), side="right").astype(jnp.int32)
    table = members.reshape(top, rows).T
    table = table[jax.random.permutation(jax.random.fold_in(own, 1), rows)]
    offset_by = jax.random.randint(jax.random.fold_in(own, 2), (rows, 1), 0, top)
    return jnp.take_along_axis(table, (jnp.arange(top)[None, :] + offset_by) % top, axis=1)


def portions_of(number_of, total, limit, slope, full):
    weights = [(1 << 20) // math.isqrt(grade ** slope) + 1 for grade in range(1, number_of + 1)]
    largest = limit if full else min(limit, max(-(-total // number_of), total * weights[0] // sum(weights)))
    least = 1 if total - largest >= number_of - 1 else 0
    given, spare = [largest] + [least] * (number_of - 1), total - largest - least * (number_of - 1)
    while spare > 0:
        candidates = [i for i in range(1, number_of) if given[i] < largest] or [i for i in range(1, number_of) if given[i] < limit]
        whole, budget = sum([weights[i] for i in candidates]), spare
        for i in candidates:
            addition = min(limit - given[i], max(1, budget * weights[i] // whole), spare)
            given[i] = given[i] + addition
            spare = spare - addition
    return np.array(given)


def bell_draw(rng, extent, scale, limit, cuts=(), held_as=jnp.bfloat16):
    values = jax.random.normal(rng, extent, jnp.float32) * scale
    if len(cuts) > 0:
        values = steps_of(rng, extent, cuts, -0.22, 0.18) * values
    return jnp.clip(values, min=-limit, max=limit).astype(held_as)


def setup_inputs(seed: int = 0, part: int = 0) -> dict:
    keys = jax.random.split(jax.random.key(seed), 7)
    own_keys = jax.random.split(jax.random.fold_in(keys[6], part), 7)
    tokens = bell_draw(own_keys[0], (TOKENS, D), 1.0, 6.0, ((0, 16),))
    route_ids_keys = jax.random.split(jax.random.fold_in(own_keys[1], 1), TOKENS // TOK_DEV)
    route_ids_turns = jax.random.permutation(jax.random.fold_in(own_keys[1], 3), TOKENS // TOK_DEV)
    route_ids = jax.vmap(lambda own, number: shared_out(jax.random.fold_in(own_keys[1], 2), own, number, TOK_DEV, EXPERTS, TOP, CAP, 2))(route_ids_keys, route_ids_turns).reshape((TOKENS, TOP))
    levels = set_ends(jax.random.randint(own_keys[2], (TOKENS, TOP), 1, 65), jax.random.fold_in(own_keys[2], 1), 1, 64).astype(jnp.int32)
    w_gate = bell_draw(keys[3], (N_EXPERT, D, FF_DEV), D ** -0.5, 0.0625, ((0, 16),))
    w_up = bell_draw(keys[4], (N_EXPERT, D, FF_DEV), D ** -0.5, 0.0625, ((0, 16),))
    w_down = bell_draw(keys[5], (N_EXPERT, FF_DEV, D), FF_WIN ** -0.5, 0.125, ((0, 16),))
    return {"tokens": tokens, "route_ids": route_ids, "levels": levels, "w_gate": w_gate, "w_up": w_up, "w_down": w_down}


def reference(tokens, route_ids, levels, w_gate, w_up, w_down):
    total, width = tokens.shape
    top = route_ids.shape[1]
    experts = w_gate.shape[0] // SHARDS
    room = N_EXPERT * CAP
    flat_ids = route_ids.reshape(-1)
    count = flat_ids.shape[0]
    level_f = levels.astype(jnp.float32)
    weights = level_f / jnp.sum(level_f, axis=1, keepdims=True)
    flat_w = weights.reshape(-1)
    padded = jnp.concatenate([tokens, jnp.zeros((1, width), tokens.dtype)], axis=0)
    source = (jnp.arange(count, dtype=jnp.int32) // top).astype(jnp.int32)
    gates = w_gate.reshape(experts, SHARDS, width, FF_DEV)
    ups = w_up.reshape(experts, SHARDS, width, FF_DEV)
    downs = w_down.reshape(experts, SHARDS, FF_DEV, width)

    def one_expert(carry, index):
        chosen = flat_ids == index
        rank = (jnp.cumsum(chosen.astype(jnp.int32)) - 1).astype(jnp.int32)
        place = jnp.where(chosen, rank, room).astype(jnp.int32)
        owner = jnp.full((room,), total, jnp.int32).at[place].set(source, mode="drop")
        rows = padded[owner]
        summed = jnp.zeros((room, width), jnp.float32)
        for shard in range(SHARDS):
            gate = jnp.dot(rows, gates[index, shard], preferred_element_type=jnp.float32)
            up = jnp.dot(rows, ups[index, shard], preferred_element_type=jnp.float32)
            hidden = (jax.nn.silu(gate) * up).astype(jnp.bfloat16)
            part = jnp.dot(hidden, downs[index, shard], preferred_element_type=jnp.float32).astype(jnp.bfloat16)
            part = lax.optimization_barrier(part)
            summed = summed + part.astype(jnp.float32)
        rounded = summed.astype(jnp.bfloat16)
        rounded = lax.optimization_barrier(rounded)
        out_e = rounded.astype(jnp.float32)
        safe = jnp.clip(rank, 0, room - 1).astype(jnp.int32)
        picked = out_e[safe] * jnp.where(chosen, flat_w, jnp.float32(0.0))[:, None]
        return carry + jnp.sum(picked.reshape(total, top, width), axis=1), None

    start = jnp.zeros((total, width), jnp.float32)
    result, unused = lax.scan(one_expert, start, jnp.arange(experts, dtype=jnp.int32))
    return result.astype(jnp.bfloat16)
```

```python
import jax
import jax.numpy as jnp
from jax import lax
from jax.sharding import PartitionSpec as P

SHARDS = 4


def on_device(tokens, route_ids, levels, w_gate, w_up, w_down):
    tok_rows, width = tokens.shape
    top = route_ids.shape[1]
    devices = lax.axis_size("expert")
    experts = devices // SHARDS
    capacity = 5 * tok_rows * top // (4 * experts)
    f32, bf16 = jnp.float32, jnp.bfloat16

    def swap(x, distance):
        return lax.ppermute(x, "expert", [(i, i ^ distance) for i in range(devices)])

    own = lax.axis_index("expert") // SHARDS
    ids = own ^ jnp.arange(experts, dtype=jnp.int32)
    named = route_ids[:, :, None] == ids[None, None, :]
    has = jnp.any(named, axis=1)
    level_f = levels.astype(f32)
    weights = level_f / jnp.sum(level_f, axis=1, keepdims=True)
    weight = jnp.sum(jnp.where(named, weights[:, :, None], 0.0), axis=1)
    row = jnp.arange(tok_rows, dtype=jnp.int32)
    earlier = (row[None, :] < row[:, None]).astype(bf16)
    rank = jnp.dot(earlier, has.astype(bf16), preferred_element_type=f32).astype(jnp.int32)
    slots = jnp.arange(capacity, dtype=jnp.int32)
    spot = has[:, :, None] & (rank[:, :, None] == slots[None, None, :])
    weighted = jnp.where(spot, weight[:, :, None], 0.0)
    weighted_hi = weighted.astype(bf16)
    weighted_lo = (weighted - weighted_hi.astype(f32)).astype(bf16)

    batches = list(range(experts))
    gathered = {}
    for k in batches[::-1]:
        pick = spot[:, k, :].astype(bf16)
        rows = lax.dot_general(pick, tokens, (((0,), (0,)), ((), ())), preferred_element_type=f32).astype(bf16)
        gathered[k] = rows
    arrived = {k: (swap(gathered[k], SHARDS * k) if k else gathered[k]) for k in batches[::-1]}

    total = None
    for k in batches:
        near = arrived[k]
        across = swap(near, 2)
        rows = jnp.concatenate([near, across, swap(near, 1), swap(across, 1)], axis=0)
        gate = jnp.dot(rows, w_gate[0], preferred_element_type=f32)
        up = jnp.dot(rows, w_up[0], preferred_element_type=f32)
        hidden = (jax.nn.silu(gate) * up).astype(bf16)
        give = jnp.dot(hidden[2 * capacity:], w_down[0], preferred_element_type=f32).astype(bf16)
        keep = jnp.dot(hidden[: 2 * capacity], w_down[0], preferred_element_type=f32).astype(bf16)
        pair = swap(give, 1)
        far = (keep[capacity:].astype(f32) + pair[capacity:].astype(f32)).astype(bf16)
        other = swap(far, 2)
        done = (keep[:capacity].astype(f32) + pair[:capacity].astype(f32) + other.astype(f32)).astype(bf16)
        back = swap(done, SHARDS * k) if k else done
        part = jnp.dot(weighted_hi[:, k, :], back, preferred_element_type=f32)
        part = part + jnp.dot(weighted_lo[:, k, :], back, preferred_element_type=f32)
        total = part if total is None else total + part
    return total.astype(bf16)


def solution(mesh):
    return jax.shard_map(
        on_device,
        mesh=mesh,
        in_specs=(
            P(("groups", "expert"), None),
            P(("groups", "expert"), None),
            P(("groups", "expert"), None),
            P("expert", None, None),
            P("expert", None, None),
            P("expert", None, None),
        ),
        out_specs=P(("groups", "expert"), None),
        check_vma=False,
    )
```

```python
import jax
import jax.numpy as jnp
from jax import lax
from jax.sharding import PartitionSpec as P

SHARDS = 4


def plan(experts):
    sends = [2, 1] + list(range(3, experts))
    events = [("send", k) for k in sends]
    events += [("out", 0), ("pass", 0), ("mul", 0), ("out", 2), ("out", 1)]
    events += [("pass", 2), ("mul", 2), ("ret", 2), ("out", 3), ("pass", 1), ("mul", 1), ("home", 2), ("ret", 1)]
    events += [("pass", 3), ("mul", 3), ("ret", 3)]
    for k in range(4, experts):
        events += [("out", k), ("pass", k), ("mul", k), ("ret", k)]
    events += [("ret", 0), ("home", 1), ("home", 3)]
    return events + [("home", k) for k in range(4, experts)] + [("home", 0)]


def layer(tokens, route_ids, levels, w_gate, w_up, w_down):
    tok_rows, _ = tokens.shape
    top = route_ids.shape[1]
    devices = lax.axis_size("expert")
    experts = devices // SHARDS
    capacity = 5 * tok_rows * top // (4 * experts)
    f32, bf16 = jnp.float32, jnp.bfloat16

    def swap(x, distance):
        return lax.ppermute(x, "expert", [(i, i ^ distance) for i in range(devices)])

    own = lax.axis_index("expert") // SHARDS
    ids = own ^ jnp.arange(experts, dtype=jnp.int32)
    named = route_ids[:, :, None] == ids[None, None, :]
    has = jnp.any(named, axis=1)
    level_f = levels.astype(f32)
    weights = level_f / jnp.sum(level_f, axis=1, keepdims=True)
    weight = jnp.sum(jnp.where(named, weights[:, :, None], 0.0), axis=1)
    row = jnp.arange(tok_rows, dtype=jnp.int32)
    earlier = (row[None, :] < row[:, None]).astype(bf16)
    rank = jnp.dot(earlier, has.astype(bf16), preferred_element_type=f32).astype(jnp.int32)
    slots = jnp.arange(capacity, dtype=jnp.int32)
    spot = has[:, :, None] & (rank[:, :, None] == slots[None, None, :])
    weighted = jnp.where(spot, weight[:, :, None], 0.0)
    weighted_hi = weighted.astype(bf16)
    weighted_lo = (weighted - weighted_hi.astype(f32)).astype(bf16)

    mark = tokens

    def held(x):
        return lax.optimization_barrier((x, mark))[0]

    def gather(k):
        pick = spot[:, k, :].astype(bf16)
        return lax.dot_general(
            pick, held(tokens), (((0,), (0,)), ((), ())), preferred_element_type=f32
        ).astype(bf16)

    arrived, across, beside, corner, keep, pair, other, back = {}, {}, {}, {}, {}, {}, {}, {}
    for step, k in plan(experts):
        if step == "send":
            mark = gather(k)
            arrived[k] = swap(mark, SHARDS * k)
        elif step == "out":
            arrived[k] = mark = held(arrived[k]) if k else gather(k)
            across[k] = swap(mark, 2)
            beside[k] = swap(mark, 1)
        elif step == "pass":
            across[k] = mark = held(across[k])
            corner[k] = swap(mark, 1)
        elif step == "mul":
            rows = jnp.concatenate([arrived[k], across[k], beside[k], corner[k]], axis=0)
            rows = held(rows)
            gate = jnp.dot(rows, w_gate[0], preferred_element_type=f32)
            up = jnp.dot(rows, w_up[0], preferred_element_type=f32)
            hidden = (jax.nn.silu(gate) * up).astype(bf16)
            mark = jnp.dot(hidden[2 * capacity:], w_down[0], preferred_element_type=f32).astype(bf16)
            pair[k] = swap(mark, 1)
            keep[k] = jnp.dot(hidden[: 2 * capacity], w_down[0], preferred_element_type=f32).astype(bf16)
        elif step == "ret":
            pair[k] = held(pair[k])
            mark = (keep[k][capacity:].astype(f32) + pair[k][capacity:].astype(f32)).astype(bf16)
            other[k] = swap(mark, 2)
        else:
            came = held(other[k])
            mark = (
                keep[k][:capacity].astype(f32) + pair[k][:capacity].astype(f32) + came.astype(f32)
            ).astype(bf16)
            back[k] = swap(mark, SHARDS * k) if k else mark

    total = None
    for k in [k for step, k in plan(experts) if step == "home"]:
        part = jnp.dot(weighted_hi[:, k, :], back[k], preferred_element_type=f32)
        part = part + jnp.dot(weighted_lo[:, k, :], back[k], preferred_element_type=f32)
        total = part if total is None else total + part
    return total.astype(bf16)


def solution(mesh):
    return jax.shard_map(
        layer,
        mesh=mesh,
        in_specs=(
            P(("groups", "expert"), None),
            P(("groups", "expert"), None),
            P(("groups", "expert"), None),
            P("expert", None, None),
            P("expert", None, None),
            P("expert", None, None),
        ),
        out_specs=P(("groups", "expert"), None),
        check_vma=False,
    )
```
